512 devices in a mesh: tm: 128 (over x, z, y_hi), cuts: 4 (over y_lo, core).
Axes of the slice: x: 4, y: 4 (y_hi: 2, y_lo: 2; y = y_hi * 2 + y_lo), z: 16, core: 2. Of those that a mesh axis runs over, the one named last changes fastest.
Arguments:
- start_image: float32 [512, 2, 128, 256], P(('cuts', 'tm')), parts along dimension 0, may hold values from -6 to 6
- sensitivity: bfloat16 [32, 2, 128, 256], P('cuts'), parts along dimension 0, may hold values from -2 to 2
- kspace: bfloat16 [512, 8, 2, 128, 256], P(('cuts', 'tm')), parts along dimension 0, may hold values from -6 to 6
- sampled: int32 [512, 8, 256], P(('cuts', 'tm')), parts along dimension 0, may hold values from 0 to 1
- offsets: int32 [8, 2], P('cuts'), parts along dimension 0, may hold values from 0 to 15
Outputs:
- reconstruction: float32 [512, 2, 128, 256], P(('cuts', 'tm')), parts along dimension 0
The draws below stay inside these ranges and needn't reach their ends.
There are 4 independent parts, one for each index of `cuts`. The reference program is written for one: setup_inputs(seed, part) draws one part's arguments, and reference() takes and returns one part's arrays. A program takes and returns all parts, laid end to end along the dimension named above; each array names one. Nothing has to cross between parts.
All inputs are finite; a program needn't handle non-finite values. Where the reference program divides by a largest or mean magnitude, that divisor is 1e-20 or more.
Results may differ from the reference program's by a relative error of at most 0.0037.
Values sent between devices are 32-bit elements; how exact they have to be, the bound alone decides.
A program may use at most 64 MiB of HBM per device.

```python
import math
import jax
import jax.numpy as jnp
from jax import lax

NY = 256
COILS = 8
XW = 128
BS = 16
ITERS = 2
NEWTON = 4
FRAMES = 128


def draw_sampled(key, part):
    levels = jax.random.randint(jax.random.fold_in(key, 11), (FRAMES, COILS, NY), 0, 1000)
    frame_index = jnp.arange(FRAMES, dtype=jnp.int32)
    limits = 150 + 450 * frame_index // max(FRAMES - 1, 1)
    return (levels < limits[:, None, None]).astype(jnp.int32)


def plant(values, key, low, largest):
    extent = values.shape
    place = [jax.random.randint(jax.random.fold_in(key, axis), (), 0, extent[axis]) for axis in range(len(extent))]
    values = values.at[tuple(place)].set(low)
    longest = extent.index(max(extent))
    place[longest] = (place[longest] + 1) % extent[longest]
    return values.at[tuple(place)].set(largest)


def shard_levels(stream_key, extent, pieces, least, largest):
    factor_of, own = 1.0, jax.random.fold_in(stream_key, 6)
    for position, blocks in pieces:
        steps = jnp.exp(jax.random.uniform(jax.random.fold_in(own, position), (blocks,), jnp.float32, least / len(pieces), largest / len(pieces)))
        factor_of = factor_of * jnp.repeat(steps, extent[position] // blocks).reshape([-1 if axis == position else 1 for axis in range(len(extent))])
    return factor_of


def bell_draw(own_key, dims, scale, bound, split=(), kind=jnp.bfloat16):
    result = scale * jax.random.normal(own_key, dims, jnp.float32)
    if split:
        result = result * shard_levels(own_key, dims, split, -0.22, 0.18)
    return jnp.clip(result, -bound, bound).astype(kind)


def setup_inputs(seed: int = 0, part: int = 0) -> dict:
    key_of = jax.random.split(jax.random.key(seed), 6)
    part_keys = jax.random.split(jax.random.fold_in(key_of[5], part), 6)
    return {
        "start_image": bell_draw(part_keys[0], (FRAMES, 2, XW, NY), 1.0, 6.0, ((0, 128),), jnp.float32),
        "sensitivity": bell_draw(part_keys[1], (COILS, 2, XW, NY), 0.35, 2.0),
        "kspace": bell_draw(part_keys[2], (FRAMES, COILS, 2, XW, NY), 1.0, 6.0, ((0, 128),)),
        "sampled": draw_sampled(jax.random.fold_in(jax.random.fold_in(key_of[5], part), 71), part),
        "offsets": plant(jax.random.randint(part_keys[4], (ITERS, 2), 0, BS), jax.random.fold_in(part_keys[4], 1), 0, BS - 1).astype(jnp.int32),
    }


shrink_ratio = 0.5
epsilon = 1e-06

def dft_tables(length):
    indices = jnp.arange(length, dtype=jnp.int32)
    phases = indices[:, None] * indices[None, :] % length
    angles = phases.astype(jnp.float32) * (2.0 * math.pi / length)
    norm_scale = 1.0 / math.sqrt(length)
    return ((jnp.cos(angles) * norm_scale).astype(jnp.bfloat16), (jnp.sin(angles) * norm_scale).astype(jnp.bfloat16))

def forward(real_part, imag_part, cosine_table, sine_table):
    out_real = jnp.dot(real_part, cosine_table, preferred_element_type=jnp.float32) + jnp.dot(imag_part, sine_table, preferred_element_type=jnp.float32)
    out_imag = jnp.dot(imag_part, cosine_table, preferred_element_type=jnp.float32) - jnp.dot(real_part, sine_table, preferred_element_type=jnp.float32)
    return (out_real, out_imag)

def inverse(real_part, imag_part, cosine_table, sine_table):
    out_real = jnp.dot(real_part, cosine_table, preferred_element_type=jnp.float32) - jnp.dot(imag_part, sine_table, preferred_element_type=jnp.float32)
    out_imag = jnp.dot(imag_part, cosine_table, preferred_element_type=jnp.float32) + jnp.dot(real_part, sine_table, preferred_element_type=jnp.float32)
    return (out_real, out_imag)

def coil_spectra(field, sens_real, sens_imag, cosine_table, sine_table):
    coils, width, length = sens_real.shape
    coil_real = (sens_real * field[0] - sens_imag * field[1]).astype(jnp.bfloat16).reshape(coils * width, length)
    coil_imag = (sens_real * field[1] + sens_imag * field[0]).astype(jnp.bfloat16).reshape(coils * width, length)
    spec_real, spec_imag = forward(coil_real, coil_imag, cosine_table, sine_table)
    return (spec_real.reshape(coils, width, length), spec_imag.reshape(coils, width, length))

def frame_terms(field, sensitivity, data, lines, cosine_table, sine_table):
    sens_real = sensitivity[:, 0].astype(jnp.float32)
    sens_imag = sensitivity[:, 1].astype(jnp.float32)
    coils, width, length = sens_real.shape
    weight = lines.astype(jnp.float32)[:, None, :]
    spec_real, spec_imag = coil_spectra(field, sens_real, sens_imag, cosine_table, sine_table)
    misfit_real = (weight * (spec_real - data[:, 0].astype(jnp.float32))).astype(jnp.bfloat16)
    misfit_imag = (weight * (spec_imag - data[:, 1].astype(jnp.float32))).astype(jnp.bfloat16)
    back_real, back_imag = inverse(misfit_real.reshape(coils * width, length), misfit_imag.reshape(coils * width, length), cosine_table, sine_table)
    back_real = back_real.reshape(coils, width, length)
    back_imag = back_imag.reshape(coils, width, length)
    grad_real = lax.optimization_barrier(jnp.sum(sens_real * back_real + sens_imag * back_imag, axis=0))
    grad_imag = lax.optimization_barrier(jnp.sum(sens_real * back_imag - sens_imag * back_real, axis=0))
    gradient = jnp.stack([grad_real, grad_imag])
    numerator = jnp.sum(gradient * gradient)
    probe_real, probe_imag = coil_spectra(gradient, sens_real, sens_imag, cosine_table, sine_table)
    denominator = jnp.sum(weight * (probe_real * probe_real + probe_imag * probe_imag))
    return (gradient, numerator, denominator)

def shrink(casorati):
    highest = lax.Precision.HIGHEST
    gram = jnp.einsum('bfv,bgv->bfg', casorati, casorati, precision=highest)
    frames = gram.shape[1]
    identity = jnp.eye(frames, dtype=jnp.float32)
    shrink_level = shrink_ratio * jnp.trace(gram, axis1=1, axis2=2) / frames + epsilon
    system = gram + shrink_level[:, None, None] * identity
    row_bound = lax.optimization_barrier(jnp.max(lax.optimization_barrier(jnp.sum(jnp.abs(system), axis=2)), axis=1))
    approx = identity[None] / row_bound[:, None, None]
    for newton in range(NEWTON):
        product = jnp.einsum('bfg,bgh->bfh', system, approx, precision=highest)
        approx = jnp.einsum('bfg,bgh->bfh', approx, 2.0 * identity - product, precision=highest)
    return casorati - shrink_level[:, None, None] * jnp.einsum('bfg,bgv->bfv', approx, casorati, precision=highest)

def to_blocks(field):
    frames, parts, width, length = field.shape
    blocks = field.reshape(frames, parts, width // BS, BS, length // BS, BS)
    blocks = blocks.transpose(2, 4, 0, 1, 3, 5)
    return blocks.reshape(width // BS * (length // BS), frames, parts * BS * BS)

def from_blocks(blocks, width, length):
    frames = blocks.shape[1]
    field = blocks.reshape(width // BS, length // BS, frames, 2, BS, BS)
    field = field.transpose(2, 3, 0, 4, 1, 5)
    return field.reshape(frames, 2, width, length)

def reference(start_image, sensitivity, kspace, sampled, offsets):
    width, length = (start_image.shape[2], start_image.shape[3])
    cosine_table, sine_table = dft_tables(length)
    estimate = start_image

    def per_frame(frame_items):
        field, data, lines = frame_items
        return frame_terms(field, sensitivity, data, lines, cosine_table, sine_table)
    for iteration in range(ITERS):
        gradient, numerator, denominator = lax.map(per_frame, (estimate, kspace, sampled))
        step_length = jnp.sum(numerator) / (jnp.sum(denominator) + epsilon)
        moved = estimate - step_length * gradient
        offset_pair = offsets[iteration]
        rolled = jnp.roll(moved, (offset_pair[0], offset_pair[1]), axis=(2, 3))
        shrunk = shrink(to_blocks(rolled))
        placed = from_blocks(shrunk, width, length)
        estimate = jnp.roll(placed, (-offset_pair[0], -offset_pair[1]), axis=(2, 3))
    return estimate
```

```python
import functools
import math

import jax
import jax.numpy as jnp
import numpy as np
from jax import lax
from jax.experimental import pallas as pl
from jax.experimental.pallas import tpu as pltpu
from jax.sharding import PartitionSpec as P

BS = 16
LANES = 128
PER_TILE = LANES // BS
ROWS = 32
shrink_ratio = 0.5
epsilon = 1e-06
HIGHEST = lax.Precision.HIGHEST
F32 = jnp.float32
BF16 = jnp.bfloat16


def dft_matrices(length):
    indices = np.arange(length, dtype=np.int64)
    phases = (indices[:, None] * indices[None, :]) % length
    angles = phases.astype(np.float32) * np.float32(2.0 * math.pi / length)
    norm_scale = np.float32(1.0 / math.sqrt(length))
    cosine = jnp.asarray(np.cos(angles) * norm_scale).astype(BF16)
    sine = jnp.asarray(np.sin(angles) * norm_scale).astype(BF16)
    ahead = jnp.block([[cosine, -sine], [sine, cosine]])
    back = jnp.block([[cosine, sine], [-sine, cosine]])
    return ahead, back


def swap_groups(x):
    rows, lanes = x.shape
    row = lax.broadcasted_iota(jnp.int32, x.shape, 0)
    lane = lax.broadcasted_iota(jnp.int32, x.shape, 1)
    for bit in (1, 2, 4):
        low_row = (row & bit) == 0
        low_lane = (lane & (bit * BS)) == 0
        from_below = pltpu.roll(pltpu.roll(x, rows - bit, 0), bit * BS, 1)
        from_above = pltpu.roll(pltpu.roll(x, bit, 0), lanes - bit * BS, 1)
        x = jnp.where(low_row == low_lane, x, jnp.where(low_row, from_below, from_above))
    return x


def kernel(
    sizes, iters, newton,
    start, sens, kspace, sampled, offsets, ahead, back,
    out,
    field, grad, sums_src, sums, casorati_src, casorati, shrunk_src, shrunk,
    send_sems, recv_sems,
):
    nx, nz, ny = sizes
    count = nx * nz * ny
    coils, _, width, length = sens.shape
    halves = length // LANES
    per_row = length // BS
    me = lax.axis_index("tm")
    my_x, my_z, my_y = me // (nz * ny), (me // ny) % nz, me % ny
    barrier = pltpu.get_barrier_semaphore()

    def peers(act):
        def at_distance(i, skip_self):
            hop = nz // 2 + (1 - 2 * (i % 2)) * ((i + 1) // 2)
            z = (my_z + hop) % nz
            for dx in range(nx):
                for dy in range(ny):
                    if skip_self and dx == 0 and dy == 0:
                        continue
                    act((((my_x + dx) % nx) * nz + z) * ny + (my_y + dy) % ny)

        def body(i, carry):
            at_distance(i, False)
            return carry

        lax.fori_loop(0, nz - 1, body, 0)
        at_distance(nz - 1, True)

    peers(lambda peer: pl.semaphore_signal(barrier, inc=1, device_id={"tm": peer}))

    field[...] = start[...]
    weight = sampled[...].astype(F32)[:, None, :]

    def exchange(src_of, dst, phase, it):
        def send(peer):
            pltpu.make_async_remote_copy(
                src_ref=src_of(peer),
                dst_ref=dst.at[it, me],
                send_sem=send_sems.at[phase, it],
                recv_sem=recv_sems.at[phase, it],
                device_id={"tm": peer},
            ).start()

        peers(send)

    def all_of(dst, phase, it):
        whole = dst.at[it, pl.ds(0, count - 1)]
        return pltpu.make_async_remote_copy(
            src_ref=whole, dst_ref=whole, send_sem=send_sems.at[phase, it],
            recv_sem=recv_sems.at[phase, it], device_id={"tm": me},
        )

    def iteration(it, carry):
        def chunk(c, acc):
            num, den = acc
            r0 = pl.multiple_of(c * ROWS, ROWS)
            here = pl.ds(r0, ROWS)
            sr = sens[:, 0, here, :].astype(F32)
            si = sens[:, 1, here, :].astype(F32)

            def spectra(re, im):
                cr = (sr * re - si * im).astype(BF16).reshape(coils * ROWS, length)
                ci = (sr * im + si * re).astype(BF16).reshape(coils * ROWS, length)
                spec = jnp.dot(
                    jnp.concatenate([cr, ci], axis=1), ahead[...], preferred_element_type=F32
                )
                return (
                    spec[:, :length].reshape(coils, ROWS, length),
                    spec[:, length:].reshape(coils, ROWS, length),
                )

            fr, fi = spectra(field[0, here, :], field[1, here, :])
            mr = (weight * (fr - kspace[:, 0, here, :].astype(F32))).astype(BF16)
            mi = (weight * (fi - kspace[:, 1, here, :].astype(F32))).astype(BF16)
            misfit = jnp.concatenate(
                [mr.reshape(coils * ROWS, length), mi.reshape(coils * ROWS, length)], axis=1
            )
            image = jnp.dot(misfit, back[...], preferred_element_type=F32)
            br = image[:, :length].reshape(coils, ROWS, length)
            bi = image[:, length:].reshape(coils, ROWS, length)
            gr = jnp.sum(sr * br + si * bi, axis=0)
            gi = jnp.sum(sr * bi - si * br, axis=0)
            grad[0, here, :] = gr
            grad[1, here, :] = gi
            num = num + jnp.sum((gr * gr + gi * gi).reshape(ROWS // 8, 8, length), axis=0)
            pr, pi = spectra(gr, gi)
            power = jnp.sum(weight * (pr * pr + pi * pi), axis=0)
            den = den + jnp.sum(power.reshape(ROWS // 8, 8, length), axis=0)
            return num, den

        zero = jnp.zeros((8, length), F32)
        num, den = lax.fori_loop(0, width // ROWS, chunk, (zero, zero))

        def fold(v):
            v = jnp.sum(v, axis=0, keepdims=True)
            v = sum(v[:, h * LANES : (h + 1) * LANES] for h in range(halves))
            return v + pltpu.roll(v, LANES // 2, 1)

        first = lax.broadcasted_iota(jnp.int32, (1, LANES), 1) < LANES // 2
        mine = jnp.where(first, fold(num), fold(den))
        sums_src[it] = mine
        sums[it, me] = mine

        @pl.when(it == 0)
        def _():
            pl.semaphore_wait(barrier, count - 1)

        exchange(lambda peer: sums_src.at[it], sums, 0, it)
        all_of(sums, 0, it).wait_recv()
        total = jnp.sum(sums[it], axis=0)
        num_all = jnp.sum(jnp.where(first, total, 0.0), axis=1, keepdims=True)
        den_all = jnp.sum(jnp.where(first, 0.0, total), axis=1, keepdims=True)
        step_length = num_all / (den_all + epsilon)

        shift_x, shift_y = offsets[it, 0], offsets[it, 1]
        for p in range(2):
            moved = field[p] - step_length * grad[p]
            rolled = pltpu.roll(pltpu.roll(moved, shift_x, 0), shift_y, 1)
            for h in range(halves):
                swapped = swap_groups(rolled[:, h * LANES : (h + 1) * LANES])
                for g in range(width // 8):
                    u, q = g // 2, g % 2
                    rows = pl.ds(u * per_row + h * PER_TILE, PER_TILE)
                    casorati_src[it, rows, p * 2 + q, :] = swapped[g * 8 : (g + 1) * 8, :]

        exchange(lambda peer: casorati_src.at[it, peer], casorati, 1, it)
        casorati[it, me] = casorati_src[it, me]
        all_of(casorati, 1, it).wait_recv()

        parts = [casorati[it, :, j, :] for j in range(4)]
        contract_last = (((1,), (1,)), ((), ()))
        full = jnp.concatenate(parts, axis=1)
        gram = lax.dot_general(
            full, full, contract_last, precision=HIGHEST, preferred_element_type=F32
        )
        frames = gram.shape[0]
        eye = (
            lax.broadcasted_iota(jnp.int32, gram.shape, 0)
            == lax.broadcasted_iota(jnp.int32, gram.shape, 1)
        ).astype(F32)
        trace = jnp.sum(jnp.sum(gram * eye, axis=1, keepdims=True), axis=0, keepdims=True)
        level = shrink_ratio * trace / frames + epsilon
        system = gram + level * eye
        bound = jnp.max(jnp.sum(jnp.abs(system), axis=1, keepdims=True), axis=0, keepdims=True)

        def times(a, b):
            return jnp.dot(a, b, precision=HIGHEST, preferred_element_type=F32)

        residual = eye - system / bound
        product = eye + residual
        power = times(residual, residual)
        for step in range(newton - 2):
            both = times(jnp.concatenate([power, product], axis=0), power)
            product = product + both[frames:]
            power = both[:frames]
        product = product + times(product, power)
        scaled = product * (level / bound)
        result = full - times(scaled, full)
        for j in range(4):
            shrunk_src[it, :, j, :] = result[:, j * LANES : (j + 1) * LANES]

        exchange(lambda peer: shrunk_src.at[it, peer], shrunk, 2, it)
        shrunk[it, me] = shrunk_src[it, me]
        all_of(shrunk, 2, it).wait_recv()

        for p in range(2):
            columns = []
            for h in range(halves):
                tiles = []
                for g in range(width // 8):
                    u, q = g // 2, g % 2
                    rows = pl.ds(u * per_row + h * PER_TILE, PER_TILE)
                    tiles.append(shrunk[it, rows, p * 2 + q, :])
                columns.append(swap_groups(jnp.concatenate(tiles, axis=0)))
            placed = jnp.concatenate(columns, axis=1)
            field[p] = pltpu.roll(pltpu.roll(placed, width - shift_x, 0), length - shift_y, 1)

        for phase, dst in enumerate((sums, casorati, shrunk)):
            all_of(dst, phase, it).wait_send()
        return carry

    lax.fori_loop(0, iters, iteration, 0)
    out[...] = field[...]


def body(sizes, start_image, sensitivity, kspace, sampled, offsets):
    iters = offsets.shape[0]
    newton = 4
    _, _, width, length = start_image.shape
    coils = sensitivity.shape[0]
    count = sizes[0] * sizes[1] * sizes[2]
    ahead, back = dft_matrices(length)
    vmem = pl.BlockSpec(memory_space=pltpu.VMEM)
    run = pl.pallas_call(
        functools.partial(kernel, sizes, iters, newton),
        name="reconstruct",
        out_shape=jax.ShapeDtypeStruct((2, width, length), F32),
        in_specs=[vmem, vmem, vmem, vmem, pl.BlockSpec(memory_space=pltpu.SMEM), vmem, vmem],
        out_specs=vmem,
        scratch_shapes=[
            pltpu.VMEM((2, width, length), F32),
            pltpu.VMEM((2, width, length), F32),
            pltpu.VMEM((iters, 1, LANES), F32),
            pltpu.VMEM((iters, count, 1, LANES), F32),
            pltpu.VMEM((iters, count, 4, LANES), F32),
            pltpu.VMEM((iters, count, 4, LANES), F32),
            pltpu.VMEM((iters, count, 4, LANES), F32),
            pltpu.VMEM((iters, count, 4, LANES), F32),
            pltpu.SemaphoreType.DMA((3, iters)),
            pltpu.SemaphoreType.DMA((3, iters)),
        ],
        compiler_params=pltpu.CompilerParams(
            collective_id=0, has_side_effects=True, vmem_limit_bytes=48 * 2**20
        ),
    )
    result = run(start_image[0], sensitivity, kspace[0], sampled[0], offsets, ahead, back)
    return result[None]


def solution(mesh):
    count = mesh.shape["tm"]
    sizes = (4, count // 8, 2) if count >= 64 else (2, count // 4, 2)
    both = ("cuts", "tm")
    placed = (
        P(both, None, None, None),
        P("cuts", None, None, None),
        P(both, None, None, None, None),
        P(both, None, None),
        P("cuts", None),
    )
    return jax.shard_map(
        functools.partial(body, sizes), mesh=mesh, in_specs=placed,
        out_specs=P(both, None, None, None), check_vma=False,
    )
```

```python
import functools
import math

import jax
import jax.numpy as jnp
import numpy as np
from jax import lax
from jax.experimental import pallas as pl
from jax.experimental.pallas import tpu as pltpu
from jax.sharding import PartitionSpec as P

BS = 16
LANES = 128
PER_TILE = LANES // BS
ROWS = 64
EARLY = 0
CLASSES = 2
shrink_ratio = 0.5
epsilon = 1e-06
F32 = jnp.float32
BF16 = jnp.bfloat16


def dft_matrices(length):
    indices = np.arange(length, dtype=np.int64)
    phases = (indices[:, None] * indices[None, :]) % length
    angles = phases.astype(np.float32) * np.float32(2.0 * math.pi / length)
    norm_scale = np.float32(1.0 / math.sqrt(length))
    cosine = jnp.asarray(np.cos(angles) * norm_scale).astype(BF16)
    sine = jnp.asarray(np.sin(angles) * norm_scale).astype(BF16)
    ahead = jnp.block([[cosine, -sine], [sine, cosine]])
    back = jnp.block([[cosine, sine], [-sine, cosine]])
    return ahead, back


def swap_groups(x):
    rows, lanes = x.shape
    row = lax.broadcasted_iota(jnp.int32, x.shape, 0)
    lane = lax.broadcasted_iota(jnp.int32, x.shape, 1)
    for bit in (1, 2, 4):
        low_row = (row & bit) == 0
        low_lane = (lane & (bit * BS)) == 0
        from_below = pltpu.roll(pltpu.roll(x, rows - bit, 0), bit * BS, 1)
        from_above = pltpu.roll(pltpu.roll(x, bit, 0), lanes - bit * BS, 1)
        x = jnp.where(low_row == low_lane, x, jnp.where(low_row, from_below, from_above))
    return x


def kernel(
    sizes, iters, newton,
    start_hbm, sens_hbm, kspace_hbm, sampled_hbm, offsets, ahead_hbm, back_hbm,
    out,
    sens, kspace, sampled, ahead, back,
    field, grad, sums_src, sums, held_src, held, slope_src, slope,
    casorati_src, casorati, shrunk_src, shrunk,
    load_sems, send_sems, recv_sems,
):
    nx, nz, ny = sizes
    count = nx * nz * ny
    coils, _, width, length = sens.shape
    halves = length // LANES
    per_row = length // BS
    me = lax.axis_index("tm")
    my_x, my_z, my_y = me // (nz * ny), (me // ny) % nz, me % ny
    plane = nx * ny
    reach = min(EARLY, nz - 1)
    barrier = pltpu.get_barrier_semaphore()
    loads = [
        pltpu.make_async_copy(src, dst, load_sems.at[i])
        for i, (src, dst) in enumerate(
            (
                (sampled_hbm, sampled), (start_hbm, field), (sens_hbm, sens),
                (ahead_hbm, ahead), (kspace_hbm, kspace), (back_hbm, back),
            )
        )
    ]
    for load in loads:
        load.start()

    def hop_of(i):
        return nz // 2 + (1 - 2 * (i % 2)) * ((i + 1) // 2)

    def peers(act, low=0, high=nz, classes=1):
        span = high - low

        def body(i, carry):
            z = (my_z + hop_of(low + i % span)) % nz
            for dx in range(nx // classes):
                for dy in range(ny):
                    if classes == 1:
                        x = (my_x + dx) % nx
                    else:
                        x = i // span + classes * dx
                    peer = (x * nz + z) * ny + (my_y + dy) % ny
                    if high < nz:
                        act(peer)
                    else:
                        pl.when(peer != me)(functools.partial(act, peer))
            return carry

        lax.fori_loop(0, classes * span, body, 0)

    peers(lambda peer: pl.semaphore_signal(barrier, inc=1, device_id={"tm": peer}))

    for load in loads:
        load.wait()
    weight = sampled[...].astype(F32)[:, None, :]

    def exchange(src_of, dst, phase, it, *which):
        def send(peer):
            pltpu.make_async_remote_copy(
                src_ref=src_of(peer),
                dst_ref=dst.at[it, me],
                send_sem=send_sems.at[phase, it],
                recv_sem=recv_sems.at[phase, it],
                device_id={"tm": peer},
            ).start()

        peers(send, *which)

    def all_of(dst, phase, it, amount):
        whole = dst.at[it, pl.ds(0, amount)]
        return pltpu.make_async_remote_copy(
            src_ref=whole, dst_ref=whole, send_sem=send_sems.at[phase, it],
            recv_sem=recv_sems.at[phase, it], device_id={"tm": me},
        )

    def iteration(it, carry):
        def chunk(c, acc):
            num, den = acc
            r0 = pl.multiple_of(c * ROWS, ROWS)
            here = pl.ds(r0, ROWS)
            sr = sens[:, 0, here, :].astype(F32)
            si = sens[:, 1, here, :].astype(F32)

            def spectra(re, im):
                cr = (sr * re - si * im).astype(BF16).reshape(coils * ROWS, length)
                ci = (sr * im + si * re).astype(BF16).reshape(coils * ROWS, length)
                spec = jnp.dot(
                    jnp.concatenate([cr, ci], axis=1), ahead[...], preferred_element_type=F32
                )
                return (
                    spec[:, :length].reshape(coils, ROWS, length),
                    spec[:, length:].reshape(coils, ROWS, length),
                )

            fr, fi = spectra(field[0, here, :], field[1, here, :])
            mr = (weight * (fr - kspace[:, 0, here, :].astype(F32))).astype(BF16)
            mi = (weight * (fi - kspace[:, 1, here, :].astype(F32))).astype(BF16)
            misfit = jnp.concatenate(
                [mr.reshape(coils * ROWS, length), mi.reshape(coils * ROWS, length)], axis=1
            )
            image = jnp.dot(misfit, back[...], preferred_element_type=F32)
            br = image[:, :length].reshape(coils, ROWS, length)
            bi = image[:, length:].reshape(coils, ROWS, length)
            gr = jnp.sum(sr * br + si * bi, axis=0)
            gi = jnp.sum(sr * bi - si * br, axis=0)
            grad[0, here, :] = gr
            grad[1, here, :] = gi
            num = num + jnp.sum((gr * gr + gi * gi).reshape(ROWS // 8, 8, length), axis=0)
            pr, pi = spectra(gr, gi)
            power = jnp.sum(weight * (pr * pr + pi * pi), axis=0)
            den = den + jnp.sum(power.reshape(ROWS // 8, 8, length), axis=0)
            return num, den

        zero = jnp.zeros((8, length), F32)
        num, den = lax.fori_loop(0, width // ROWS, chunk, (zero, zero))

        def fold(v):
            v = jnp.sum(v, axis=0, keepdims=True)
            v = sum(v[:, h * LANES : (h + 1) * LANES] for h in range(halves))
            return v + pltpu.roll(v, LANES // 2, 1)

        first = lax.broadcasted_iota(jnp.int32, (1, LANES), 1) < LANES // 2
        mine = jnp.where(first, fold(num), fold(den))
        sums_src[it] = mine
        sums[it, me] = mine

        @pl.when(it == 0)
        def _():
            pl.semaphore_wait(barrier, count - 1)

        exchange(lambda peer: sums_src.at[it], sums, 0, it)

        shift_x, shift_y = offsets[it, 0], offsets[it, 1]

        def lay_out(image, dst):
            for p in range(2):
                rolled = pltpu.roll(pltpu.roll(image[p], shift_x, 0), shift_y, 1)
                for h in range(halves):
                    swapped = swap_groups(rolled[:, h * LANES : (h + 1) * LANES])
                    for g in range(width // 8):
                        u, q = g // 2, g % 2
                        rows = pl.ds(u * per_row + h * PER_TILE, PER_TILE)
                        dst[it, rows, p * 2 + q, :] = swapped[g * 8 : (g + 1) * 8, :]

        lay_out(field, held_src)
        if reach:
            exchange(lambda peer: held_src.at[it, peer], held, 1, it, 0, reach)
        lay_out(grad, slope_src)
        if reach:
            exchange(lambda peer: slope_src.at[it, peer], slope, 2, it, 0, reach)

        all_of(sums, 0, it, count - 1).wait_recv()
        total = jnp.sum(sums[it], axis=0)
        num_all = jnp.sum(jnp.where(first, total, 0.0), axis=1, keepdims=True)
        den_all = jnp.sum(jnp.where(first, 0.0, total), axis=1, keepdims=True)
        step_length = num_all / (den_all + epsilon)

        casorati_src[it] = held_src[it] - step_length[None] * slope_src[it]
        exchange(
            lambda peer: casorati_src.at[it, peer], casorati, 3, it, reach, nz, CLASSES
        )
        casorati[it, me] = casorati_src[it, me]
        if reach:
            all_of(held, 1, it, reach * plane).wait_recv()
            all_of(slope, 2, it, reach * plane).wait_recv()
        all_of(casorati, 3, it, count - 1 - reach * plane).wait_recv()
        for k in range(reach):
            z = (my_z + hop_of(k)) % nz
            for x in range(nx):
                rows = pl.ds((x * nz + z) * ny, ny)
                casorati[it, rows] = held[it, rows] - step_length[None] * slope[it, rows]

        parts = [casorati[it, :, j, :] for j in range(4)]
        full = jnp.concatenate(parts, axis=1)

        def split(a):
            high = a.astype(BF16)
            return high, (a - high.astype(F32)).astype(BF16)

        full_high, full_low = split(full)
        gram = lax.dot_general(
            jnp.concatenate([full_high, full_low, full_high], axis=1),
            jnp.concatenate([full_high, full_high, full_low], axis=1),
            (((1,), (1,)), ((), ())), preferred_element_type=F32,
        )
        frames = gram.shape[0]
        eye = (
            lax.broadcasted_iota(jnp.int32, gram.shape, 0)
            == lax.broadcasted_iota(jnp.int32, gram.shape, 1)
        ).astype(F32)
        trace = jnp.sum(jnp.sum(gram * eye, axis=1, keepdims=True), axis=0, keepdims=True)
        level = shrink_ratio * trace / frames + epsilon
        system = gram + level * eye
        bound = jnp.max(jnp.sum(jnp.abs(system), axis=1, keepdims=True), axis=0, keepdims=True)

        def times(a, b):
            a_high, a_low = split(a)
            b_high, b_low = split(b)
            return jnp.dot(
                jnp.concatenate([a_high, a_low, a_high], axis=1),
                jnp.concatenate([b_high, b_high, b_low], axis=0),
                preferred_element_type=F32,
            )

        residual = eye - system / bound
        product = eye + residual
        power = times(residual, residual)
        for step in range(newton - 2):
            both = times(jnp.concatenate([power, product], axis=0), power)
            product = product + both[frames:]
            power = both[:frames]
        product = product + times(product, power)
        scaled = product * (level / bound)
        result = full - times(scaled, full)
        for j in range(4):
            shrunk_src[it, :, j, :] = result[:, j * LANES : (j + 1) * LANES]

        exchange(lambda peer: shrunk_src.at[it, peer], shrunk, 4, it)
        shrunk[it, me] = shrunk_src[it, me]
        all_of(shrunk, 4, it, count - 1).wait_recv()

        for p in range(2):
            columns = []
            for h in range(halves):
                tiles = []
                for g in range(width // 8):
                    u, q = g // 2, g % 2
                    rows = pl.ds(u * per_row + h * PER_TILE, PER_TILE)
                    tiles.append(shrunk[it, rows, p * 2 + q, :])
                columns.append(swap_groups(jnp.concatenate(tiles, axis=0)))
            placed = jnp.concatenate(columns, axis=1)
            field[p] = pltpu.roll(pltpu.roll(placed, width - shift_x, 0), length - shift_y, 1)

        early = reach * plane
        for phase, dst, amount in (
            (0, sums, count - 1), (1, held, early), (2, slope, early),
            (3, casorati, count - 1 - early), (4, shrunk, count - 1),
        ):
            if amount:
                all_of(dst, phase, it, amount).wait_send()
        return carry

    lax.fori_loop(0, iters, iteration, 0)
    out[...] = field[...]


def body(sizes, start_image, sensitivity, kspace, sampled, offsets):
    iters = offsets.shape[0]
    newton = 4
    _, _, width, length = start_image.shape
    coils = sensitivity.shape[0]
    count = sizes[0] * sizes[1] * sizes[2]
    ahead, back = dft_matrices(length)
    vmem = pl.BlockSpec(memory_space=pltpu.VMEM)
    hbm = pl.BlockSpec(memory_space=pltpu.HBM)
    messages = pltpu.VMEM((iters, count, 4, LANES), F32)
    run = pl.pallas_call(
        functools.partial(kernel, sizes, iters, newton),
        name="reconstruct",
        out_shape=jax.ShapeDtypeStruct((2, width, length), F32),
        in_specs=[hbm, hbm, hbm, hbm, pl.BlockSpec(memory_space=pltpu.SMEM), hbm, hbm],
        out_specs=vmem,
        scratch_shapes=[
            pltpu.VMEM(sensitivity.shape, BF16),
            pltpu.VMEM(kspace.shape[1:], BF16),
            pltpu.VMEM(sampled.shape[1:], jnp.int32),
            pltpu.VMEM(ahead.shape, BF16),
            pltpu.VMEM(back.shape, BF16),
            pltpu.VMEM((2, width, length), F32),
            pltpu.VMEM((2, width, length), F32),
            pltpu.VMEM((iters, 1, LANES), F32),
            pltpu.VMEM((iters, count, 1, LANES), F32),
            *[messages] * 8,
            pltpu.SemaphoreType.DMA((6,)),
            pltpu.SemaphoreType.DMA((5, iters)),
            pltpu.SemaphoreType.DMA((5, iters)),
        ],
        compiler_params=pltpu.CompilerParams(
            collective_id=0, has_side_effects=True, vmem_limit_bytes=48 * 2**20
        ),
    )
    result = run(start_image[0], sensitivity, kspace[0], sampled[0], offsets, ahead, back)
    return result[None]


def solution(mesh):
    count = mesh.shape["tm"]
    sizes = (4, count // 8, 2) if count >= 64 else (2, count // 4, 2)
    both = ("cuts", "tm")
    placed = (
        P(both, None, None, None),
        P("cuts", None, None, None),
        P(both, None, None, None, None),
        P(both, None, None),
        P("cuts", None),
    )
    return jax.shard_map(
        functools.partial(body, sizes), mesh=mesh, in_specs=placed,
        out_specs=P(both, None, None, None), check_vma=False,
    )
```

```python
import functools
import math

import jax
import jax.numpy as jnp
import numpy as np
from jax import lax
from jax.experimental import pallas as pl
from jax.experimental.pallas import tpu as pltpu
from jax.sharding import PartitionSpec as P

BS = 16
LANES = 128
PER_TILE = LANES // BS
ROWS = 128
EARLY = 0
CLASSES = 2
shrink_ratio = 0.5
epsilon = 1e-06
F32 = jnp.float32
BF16 = jnp.bfloat16


def dft_matrices(length):
    indices = np.arange(length, dtype=np.int64)
    phases = (indices[:, None] * indices[None, :]) % length
    angles = phases.astype(np.float32) * np.float32(2.0 * math.pi / length)
    norm_scale = np.float32(1.0 / math.sqrt(length))
    cosine = jnp.asarray(np.cos(angles) * norm_scale).astype(BF16)
    sine = jnp.asarray(np.sin(angles) * norm_scale).astype(BF16)
    ahead = jnp.block([[cosine, -sine], [sine, cosine]])
    back = jnp.block([[cosine, sine], [-sine, cosine]])
    return ahead, back


def swap_groups(x):
    rows, lanes = x.shape
    row = lax.broadcasted_iota(jnp.int32, x.shape, 0)
    lane = lax.broadcasted_iota(jnp.int32, x.shape, 1)
    for bit in (1, 2, 4):
        low_row = (row & bit) == 0
        low_lane = (lane & (bit * BS)) == 0
        from_below = pltpu.roll(pltpu.roll(x, rows - bit, 0), bit * BS, 1)
        from_above = pltpu.roll(pltpu.roll(x, bit, 0), lanes - bit * BS, 1)
        x = jnp.where(low_row == low_lane, x, jnp.where(low_row, from_below, from_above))
    return x


def kernel(
    sizes, iters, newton,
    start_hbm, sens_hbm, kspace_hbm, sampled_hbm, offsets_hbm, ahead_hbm, back_hbm,
    out,
    offsets, sens, kspace, sampled, ahead, back,
    field, grad, sums_src, sums, held_src, held, slope_src, slope,
    casorati_src, casorati, shrunk_src, shrunk,
    load_sems, send_sems, recv_sems,
):
    nx, nz, ny = sizes
    count = nx * nz * ny
    coils, _, width, length = sens.shape
    halves = length // LANES
    per_row = length // BS
    me = lax.axis_index("tm")
    my_x, my_z, my_y = me // (nz * ny), (me // ny) % nz, me % ny
    plane = nx * ny
    reach = min(EARLY, nz - 1)
    barrier = pltpu.get_barrier_semaphore()
    loads = [
        pltpu.make_async_copy(src, dst, load_sems.at[i])
        for i, (src, dst) in enumerate(
            (
                (sampled_hbm, sampled), (start_hbm, field), (sens_hbm, sens),
                (ahead_hbm, ahead), (kspace_hbm, kspace), (back_hbm, back),
                (offsets_hbm, offsets),
            )
        )
    ]
    for load in loads:
        load.start()

    def hop_of(i, flip=0):
        return nz // 2 + (1 - 2 * ((i + flip) % 2)) * ((i + 1) // 2)

    def peers(act, low=0, high=nz, classes=1):
        span = high - low

        def body(i, carry):
            for dx in range(nx // classes):
                for dy in range(ny):
                    flip = (dx * ny + dy) % 2 if low == 0 and high == nz else 0
                    z = (my_z + hop_of(low + i % span, flip)) % nz
                    if classes == 1:
                        x = (my_x + dx) % nx
                    else:
                        x = i // span + classes * dx
                    peer = (x * nz + z) * ny + (my_y + dy) % ny
                    if high < nz:
                        act(peer)
                    else:
                        pl.when(peer != me)(functools.partial(act, peer))
            return carry

        lax.fori_loop(0, classes * span, body, 0)

    peers(lambda peer: pl.semaphore_signal(barrier, inc=1, device_id={"tm": peer}))

    for load in loads[:4]:
        load.wait()
    weight = sampled[...].astype(F32)[:, None, :]

    def exchange(src_of, dst, phase, it, *which):
        def send(peer):
            pltpu.make_async_remote_copy(
                src_ref=src_of(peer),
                dst_ref=dst.at[it, me],
                send_sem=send_sems.at[phase, it],
                recv_sem=recv_sems.at[phase, it],
                device_id={"tm": peer},
            ).start()

        peers(send, *which)

    def all_of(dst, phase, it, amount):
        whole = dst.at[it, pl.ds(0, amount)]
        return pltpu.make_async_remote_copy(
            src_ref=whole, dst_ref=whole, send_sem=send_sems.at[phase, it],
            recv_sem=recv_sems.at[phase, it], device_id={"tm": me},
        )

    def iteration(it, carry):
        def chunk(c, acc):
            num, den = acc
            r0 = pl.multiple_of(c * ROWS, ROWS)
            here = pl.ds(r0, ROWS)
            sr = sens[:, 0, here, :].astype(F32)
            si = sens[:, 1, here, :].astype(F32)

            def spectra(re, im):
                cr = (sr * re - si * im).astype(BF16).reshape(coils * ROWS, length)
                ci = (sr * im + si * re).astype(BF16).reshape(coils * ROWS, length)
                spec = jnp.dot(
                    jnp.concatenate([cr, ci], axis=1), ahead[...], preferred_element_type=F32
                )
                return (
                    spec[:, :length].reshape(coils, ROWS, length),
                    spec[:, length:].reshape(coils, ROWS, length),
                )

            fr, fi = spectra(field[0, here, :], field[1, here, :])

            @pl.when((it == 0) & (c == 0))
            def _():
                for load in loads[4:]:
                    load.wait()

            mr = (weight * (fr - kspace[:, 0, here, :].astype(F32))).astype(BF16)
            mi = (weight * (fi - kspace[:, 1, here, :].astype(F32))).astype(BF16)
            misfit = jnp.concatenate(
                [mr.reshape(coils * ROWS, length), mi.reshape(coils * ROWS, length)], axis=1
            )
            image = jnp.dot(misfit, back[...], preferred_element_type=F32)
            br = image[:, :length].reshape(coils, ROWS, length)
            bi = image[:, length:].reshape(coils, ROWS, length)
            gr = jnp.sum(sr * br + si * bi, axis=0)
            gi = jnp.sum(sr * bi - si * br, axis=0)
            grad[0, here, :] = gr
            grad[1, here, :] = gi
            num = num + jnp.sum((gr * gr + gi * gi).reshape(ROWS // 8, 8, length), axis=0)
            pr, pi = spectra(gr, gi)
            power = jnp.sum(weight * (pr * pr + pi * pi), axis=0)
            den = den + jnp.sum(power.reshape(ROWS // 8, 8, length), axis=0)
            return num, den

        zero = jnp.zeros((8, length), F32)
        num, den = lax.fori_loop(0, width // ROWS, chunk, (zero, zero))

        def fold(v):
            v = jnp.sum(v, axis=0, keepdims=True)
            v = sum(v[:, h * LANES : (h + 1) * LANES] for h in range(halves))
            return v + pltpu.roll(v, LANES // 2, 1)

        first = lax.broadcasted_iota(jnp.int32, (1, LANES), 1) < LANES // 2
        mine = jnp.where(first, fold(num), fold(den))
        sums_src[it] = mine
        sums[it, me] = mine

        @pl.when(it == 0)
        def _():
            pl.semaphore_wait(barrier, count - 1)

        exchange(lambda peer: sums_src.at[it], sums, 0, it)

        shift_x, shift_y = offsets[it, 0], offsets[it, 1]

        def lay_out(image, dst):
            for p in range(2):
                rolled = pltpu.roll(pltpu.roll(image[p], shift_x, 0), shift_y, 1)
                for h in range(halves):
                    swapped = swap_groups(rolled[:, h * LANES : (h + 1) * LANES])
                    for g in range(width // 8):
                        u, q = g // 2, g % 2
                        rows = pl.ds(u * per_row + h * PER_TILE, PER_TILE)
                        dst[it, rows, p * 2 + q, :] = swapped[g * 8 : (g + 1) * 8, :]

        lay_out(field, held_src)
        if reach:
            exchange(lambda peer: held_src.at[it, peer], held, 1, it, 0, reach)
        lay_out(grad, slope_src)
        if reach:
            exchange(lambda peer: slope_src.at[it, peer], slope, 2, it, 0, reach)

        all_of(sums, 0, it, count - 1).wait_recv()
        total = jnp.sum(sums[it], axis=0)
        num_all = jnp.sum(jnp.where(first, total, 0.0), axis=1, keepdims=True)
        den_all = jnp.sum(jnp.where(first, 0.0, total), axis=1, keepdims=True)
        step_length = num_all / (den_all + epsilon)

        casorati_src[it] = held_src[it] - step_length[None] * slope_src[it]
        exchange(
            lambda peer: casorati_src.at[it, peer], casorati, 3, it, reach, nz, CLASSES
        )
        casorati[it, me] = casorati_src[it, me]
        if reach:
            all_of(held, 1, it, reach * plane).wait_recv()
            all_of(slope, 2, it, reach * plane).wait_recv()
        all_of(casorati, 3, it, count - 1 - reach * plane).wait_recv()
        for k in range(reach):
            z = (my_z + hop_of(k)) % nz
            for x in range(nx):
                rows = pl.ds((x * nz + z) * ny, ny)
                casorati[it, rows] = held[it, rows] - step_length[None] * slope[it, rows]

        parts = [casorati[it, :, j, :] for j in range(4)]
        full = jnp.concatenate(parts, axis=1)

        def split(a):
            high = a.astype(BF16)
            return high, (a - high.astype(F32)).astype(BF16)

        full_high, full_low = split(full)
        gram = lax.dot_general(
            jnp.concatenate([full_high, full_low, full_high], axis=1),
            jnp.concatenate([full_high, full_high, full_low], axis=1),
            (((1,), (1,)), ((), ())), preferred_element_type=F32,
        )
        frames = gram.shape[0]
        eye = (
            lax.broadcasted_iota(jnp.int32, gram.shape, 0)
            == lax.broadcasted_iota(jnp.int32, gram.shape, 1)
        ).astype(F32)
        trace = jnp.sum(jnp.sum(gram * eye, axis=1, keepdims=True), axis=0, keepdims=True)
        level = shrink_ratio * trace / frames + epsilon
        system = gram + level * eye
        bound = jnp.max(jnp.sum(jnp.abs(system), axis=1, keepdims=True), axis=0, keepdims=True)

        def times(a, b):
            a_high, a_low = split(a)
            b_high, b_low = split(b)
            return jnp.dot(
                jnp.concatenate([a_high, a_low, a_high], axis=1),
                jnp.concatenate([b_high, b_high, b_low], axis=0),
                preferred_element_type=F32,
            )

        residual = eye - system / bound
        product = eye + residual
        power = times(residual, residual)
        for step in range(newton - 2):
            both = times(jnp.concatenate([power, product], axis=0), power)
            product = product + both[frames:]
            power = both[:frames]
        product = product + times(product, power)
        scaled = product * (level / bound)
        result = full - times(scaled, full)
        for j in range(4):
            shrunk_src[it, :, j, :] = result[:, j * LANES : (j + 1) * LANES]

        exchange(lambda peer: shrunk_src.at[it, peer], shrunk, 4, it)
        shrunk[it, me] = shrunk_src[it, me]
        all_of(shrunk, 4, it, count - 1).wait_recv()

        for p in range(2):
            columns = []
            for h in range(halves):
                tiles = []
                for g in range(width // 8):
                    u, q = g // 2, g % 2
                    rows = pl.ds(u * per_row + h * PER_TILE, PER_TILE)
                    tiles.append(shrunk[it, rows, p * 2 + q, :])
                columns.append(swap_groups(jnp.concatenate(tiles, axis=0)))
            placed = jnp.concatenate(columns, axis=1)
            field[p] = pltpu.roll(pltpu.roll(placed, width - shift_x, 0), length - shift_y, 1)

        early = reach * plane
        for phase, dst, amount in (
            (0, sums, count - 1), (1, held, early), (2, slope, early),
            (3, casorati, count - 1 - early), (4, shrunk, count - 1),
        ):
            if amount:
                all_of(dst, phase, it, amount).wait_send()
        return carry

    lax.fori_loop(0, iters, iteration, 0)
    out[...] = field[...]


def body(sizes, start_image, sensitivity, kspace, sampled, offsets):
    iters = offsets.shape[0]
    newton = 4
    _, _, width, length = start_image.shape
    coils = sensitivity.shape[0]
    count = sizes[0] * sizes[1] * sizes[2]
    ahead, back = dft_matrices(length)
    vmem = pl.BlockSpec(memory_space=pltpu.VMEM)
    hbm = pl.BlockSpec(memory_space=pltpu.HBM)
    messages = pltpu.VMEM((iters, count, 4, LANES), F32)
    run = pl.pallas_call(
        functools.partial(kernel, sizes, iters, newton),
        name="reconstruct",
        out_shape=jax.ShapeDtypeStruct((2, width, length), F32),
        in_specs=[hbm] * 7,
        out_specs=vmem,
        scratch_shapes=[
            pltpu.SMEM(offsets.shape, jnp.int32),
            pltpu.VMEM(sensitivity.shape, BF16),
            pltpu.VMEM(kspace.shape[1:], BF16),
            pltpu.VMEM(sampled.shape[1:], jnp.int32),
            pltpu.VMEM(ahead.shape, BF16),
            pltpu.VMEM(back.shape, BF16),
            pltpu.VMEM((2, width, length), F32),
            pltpu.VMEM((2, width, length), F32),
            pltpu.VMEM((iters, 1, LANES), F32),
            pltpu.VMEM((iters, count, 1, LANES), F32),
            *[messages] * 8,
            pltpu.SemaphoreType.DMA((7,)),
            pltpu.SemaphoreType.DMA((5, iters)),
            pltpu.SemaphoreType.DMA((5, iters)),
        ],
        compiler_params=pltpu.CompilerParams(
            collective_id=0, has_side_effects=True, vmem_limit_bytes=67043328
        ),
    )
    result = run(start_image[0], sensitivity, kspace[0], sampled[0], offsets, ahead, back)
    return result[None]


def solution(mesh):
    count = mesh.shape["tm"]
    sizes = (4, count // 8, 2) if count >= 64 else (2, count // 4, 2)
    both = ("cuts", "tm")
    placed = (
        P(both, None, None, None),
        P("cuts", None, None, None),
        P(both, None, None, None, None),
        P(both, None, None),
        P("cuts", None),
    )
    return jax.shard_map(
        functools.partial(body, sizes), mesh=mesh, in_specs=placed,
        out_specs=P(both, None, None, None), check_vma=False,
    )
```

```python
import functools
import math

import jax
import jax.numpy as jnp
import numpy as np
from jax import lax
from jax.experimental import pallas as pl
from jax.experimental.pallas import tpu as pltpu
from jax.sharding import PartitionSpec as P

BS = 16
LANES = 128
PER_TILE = LANES // BS
ROWS = 128
EARLY = 1
CLASSES = 2
shrink_ratio = 0.5
epsilon = 1e-06
F32 = jnp.float32
BF16 = jnp.bfloat16


def dft_matrices(length):
    indices = np.arange(length, dtype=np.int64)
    phases = (indices[:, None] * indices[None, :]) % length
    angles = phases.astype(np.float32) * np.float32(2.0 * math.pi / length)
    norm_scale = np.float32(1.0 / math.sqrt(length))
    cosine = jnp.asarray(np.cos(angles) * norm_scale).astype(BF16)
    sine = jnp.asarray(np.sin(angles) * norm_scale).astype(BF16)
    ahead = jnp.block([[cosine, -sine], [sine, cosine]])
    back = jnp.block([[cosine, sine], [-sine, cosine]])
    return ahead, back


def swap_groups(x):
    rows, lanes = x.shape
    x = x.reshape(rows // 8, 8, lanes)
    row = lax.broadcasted_iota(jnp.int32, x.shape, 1)
    lane = lax.broadcasted_iota(jnp.int32, x.shape, 2)
    for bit in (1, 2, 4):
        low_row = (row & bit) == 0
        low_lane = (lane & (bit * BS)) == 0
        other = pltpu.roll(x, bit, 1)
        if bit < 4:
            other = jnp.where(low_row, pltpu.roll(x, 8 - bit, 1), other)
        moved = pltpu.roll(other, bit * BS, 2)
        if bit < 4:
            moved = jnp.where(low_lane, pltpu.roll(other, lanes - bit * BS, 2), moved)
        x = jnp.where(low_row == low_lane, x, moved)
    return x.reshape(rows, lanes)


def kernel(
    sizes, iters, newton,
    start_hbm, sens_hbm, kspace_hbm, sampled_hbm, offsets_hbm, ahead_hbm, back_hbm,
    out,
    offsets, sens, kspace, sampled, ahead, back,
    field, grad, sums_src, sums, held_src, held, slope_src, slope,
    casorati_src, casorati, shrunk_src, shrunk,
    load_sems, send_sems, recv_sems,
):
    nx, nz, ny = sizes
    count = nx * nz * ny
    coils, _, width, length = sens.shape
    halves = length // LANES
    per_row = length // BS
    me = lax.axis_index("tm")
    my_x, my_z, my_y = me // (nz * ny), (me // ny) % nz, me % ny
    plane = nx * ny
    reach = min(EARLY, nz - 1)
    barrier = pltpu.get_barrier_semaphore()
    loads = [
        pltpu.make_async_copy(src, dst, load_sems.at[i])
        for i, (src, dst) in enumerate(
            (
                (sampled_hbm, sampled), (start_hbm, field), (sens_hbm, sens),
                (ahead_hbm, ahead), (kspace_hbm, kspace), (back_hbm, back),
                (offsets_hbm, offsets),
            )
        )
    ]
    for load in loads:
        load.start()

    def hop_of(i, flip=0):
        return nz // 2 + (1 - 2 * ((i + flip) % 2)) * ((i + 1) // 2)

    def peers(act, low=0, high=nz, classes=1):
        span = high - low

        def body(i, carry):
            for dx in range(nx // classes):
                for dy in range(ny):
                    flip = (dx * ny + dy) % 2 if low == 0 and high == nz else 0
                    z = (my_z + hop_of(low + i % span, flip)) % nz
                    if classes == 1:
                        x = (my_x + dx) % nx
                    else:
                        x = i // span + classes * dx
                    peer = (x * nz + z) * ny + (my_y + dy) % ny
                    if high < nz:
                        act(peer)
                    else:
                        pl.when(peer != me)(functools.partial(act, peer))
            return carry

        lax.fori_loop(0, classes * span, body, 0)

    peers(lambda peer: pl.semaphore_signal(barrier, inc=1, device_id={"tm": peer}))

    for load in loads[:4]:
        load.wait()
    weight = sampled[...].astype(F32)[:, None, :]

    def exchange(src_of, dst, phase, it, *which):
        def send(peer):
            pltpu.make_async_remote_copy(
                src_ref=src_of(peer),
                dst_ref=dst.at[it, me],
                send_sem=send_sems.at[phase, it],
                recv_sem=recv_sems.at[phase, it],
                device_id={"tm": peer},
            ).start()

        peers(send, *which)

    def all_of(dst, phase, it, amount):
        whole = dst.at[it, pl.ds(0, amount)]
        return pltpu.make_async_remote_copy(
            src_ref=whole, dst_ref=whole, send_sem=send_sems.at[phase, it],
            recv_sem=recv_sems.at[phase, it], device_id={"tm": me},
        )

    def iteration(it, carry):
        def chunk(c, acc):
            num, den = acc
            r0 = pl.multiple_of(c * ROWS, ROWS)
            here = pl.ds(r0, ROWS)
            sr = sens[:, 0, here, :].astype(F32)
            si = sens[:, 1, here, :].astype(F32)

            def spectra(re, im):
                cr = (sr * re - si * im).astype(BF16).reshape(coils * ROWS, length)
                ci = (sr * im + si * re).astype(BF16).reshape(coils * ROWS, length)
                spec = jnp.dot(
                    jnp.concatenate([cr, ci], axis=1), ahead[...], preferred_element_type=F32
                )
                return (
                    spec[:, :length].reshape(coils, ROWS, length),
                    spec[:, length:].reshape(coils, ROWS, length),
                )

            fr, fi = spectra(field[0, here, :], field[1, here, :])

            @pl.when((it == 0) & (c == 0))
            def _():
                for load in loads[4:]:
                    load.wait()

            mr = (weight * (fr - kspace[:, 0, here, :].astype(F32))).astype(BF16)
            mi = (weight * (fi - kspace[:, 1, here, :].astype(F32))).astype(BF16)
            misfit = jnp.concatenate(
                [mr.reshape(coils * ROWS, length), mi.reshape(coils * ROWS, length)], axis=1
            )
            image = jnp.dot(misfit, back[...], preferred_element_type=F32)
            br = image[:, :length].reshape(coils, ROWS, length)
            bi = image[:, length:].reshape(coils, ROWS, length)
            gr = jnp.sum(sr * br + si * bi, axis=0)
            gi = jnp.sum(sr * bi - si * br, axis=0)
            grad[0, here, :] = gr
            grad[1, here, :] = gi
            num = num + jnp.sum((gr * gr + gi * gi).reshape(ROWS // 8, 8, length), axis=0)
            pr, pi = spectra(gr, gi)
            power = jnp.sum(weight * (pr * pr + pi * pi), axis=0)
            den = den + jnp.sum(power.reshape(ROWS // 8, 8, length), axis=0)
            return num, den

        zero = jnp.zeros((8, length), F32)
        num, den = lax.fori_loop(0, width // ROWS, chunk, (zero, zero))

        def fold(v):
            v = jnp.sum(v, axis=0, keepdims=True)
            v = sum(v[:, h * LANES : (h + 1) * LANES] for h in range(halves))
            return v + pltpu.roll(v, LANES // 2, 1)

        first = lax.broadcasted_iota(jnp.int32, (1, LANES), 1) < LANES // 2
        mine = jnp.where(first, fold(num), fold(den))
        sums_src[it] = mine
        sums[it, me] = mine

        @pl.when(it == 0)
        def _():
            pl.semaphore_wait(barrier, count - 1)

        exchange(lambda peer: sums_src.at[it], sums, 0, it)

        shift_x, shift_y = offsets[it, 0], offsets[it, 1]

        def lay_out(image, dst):
            for p in range(2):
                rolled = pltpu.roll(pltpu.roll(image[p], shift_x, 0), shift_y, 1)
                for h in range(halves):
                    swapped = swap_groups(rolled[:, h * LANES : (h + 1) * LANES])
                    for g in range(width // 8):
                        u, q = g // 2, g % 2
                        rows = pl.ds(u * per_row + h * PER_TILE, PER_TILE)
                        dst[it, rows, p * 2 + q, :] = swapped[g * 8 : (g + 1) * 8, :]

        lay_out(field, held_src)
        if reach:
            exchange(lambda peer: held_src.at[it, peer], held, 1, it, 0, reach)
        lay_out(grad, slope_src)
        if reach:
            exchange(lambda peer: slope_src.at[it, peer], slope, 2, it, 0, reach)

        all_of(sums, 0, it, count - 1).wait_recv()
        total = jnp.sum(sums[it], axis=0)
        num_all = jnp.sum(jnp.where(first, total, 0.0), axis=1, keepdims=True)
        den_all = jnp.sum(jnp.where(first, 0.0, total), axis=1, keepdims=True)
        step_length = num_all / (den_all + epsilon)

        casorati_src[it] = held_src[it] - step_length[None] * slope_src[it]
        exchange(
            lambda peer: casorati_src.at[it, peer], casorati, 3, it, reach, nz, CLASSES
        )
        casorati[it, me] = casorati_src[it, me]
        if reach:
            all_of(held, 1, it, reach * plane).wait_recv()
            all_of(slope, 2, it, reach * plane).wait_recv()
        all_of(casorati, 3, it, count - 1 - reach * plane).wait_recv()
        for k in range(reach):
            z = (my_z + hop_of(k)) % nz
            for x in range(nx):
                rows = pl.ds((x * nz + z) * ny, ny)
                casorati[it, rows] = held[it, rows] - step_length[None] * slope[it, rows]

        parts = [casorati[it, :, j, :] for j in range(4)]
        full = jnp.concatenate(parts, axis=1)

        def split(a):
            high = a.astype(BF16)
            return high, (a - high.astype(F32)).astype(BF16)

        full_high, full_low = split(full)
        gram = lax.dot_general(
            jnp.concatenate([full_high, full_low, full_high], axis=1),
            jnp.concatenate([full_high, full_high, full_low], axis=1),
            (((1,), (1,)), ((), ())), preferred_element_type=F32,
        )
        frames = gram.shape[0]
        eye = (
            lax.broadcasted_iota(jnp.int32, gram.shape, 0)
            == lax.broadcasted_iota(jnp.int32, gram.shape, 1)
        ).astype(F32)
        trace = jnp.sum(jnp.sum(gram * eye, axis=1, keepdims=True), axis=0, keepdims=True)
        level = shrink_ratio * trace / frames + epsilon
        system = gram + level * eye
        bound = jnp.max(jnp.sum(jnp.abs(system), axis=1, keepdims=True), axis=0, keepdims=True)

        def times(a, b):
            a_high, a_low = split(a)
            b_high, b_low = split(b)
            return jnp.dot(
                jnp.concatenate([a_high, a_low, a_high], axis=1),
                jnp.concatenate([b_high, b_high, b_low], axis=0),
                preferred_element_type=F32,
            )

        residual = eye - system / bound
        product = eye + residual
        power = times(residual, residual)
        for step in range(newton - 2):
            both = times(jnp.concatenate([power, product], axis=0), power)
            product = product + both[frames:]
            power = both[:frames]
        product = product + times(product, power)
        scaled = product * (level / bound)
        result = full - times(scaled, full)
        for j in range(4):
            shrunk_src[it, :, j, :] = result[:, j * LANES : (j + 1) * LANES]

        exchange(lambda peer: shrunk_src.at[it, peer], shrunk, 4, it)
        shrunk[it, me] = shrunk_src[it, me]
        all_of(shrunk, 4, it, count - 1).wait_recv()

        for p in range(2):
            columns = []
            for h in range(halves):
                tiles = []
                for g in range(width // 8):
                    u, q = g // 2, g % 2
                    rows = pl.ds(u * per_row + h * PER_TILE, PER_TILE)
                    tiles.append(shrunk[it, rows, p * 2 + q, :])
                columns.append(swap_groups(jnp.concatenate(tiles, axis=0)))
            placed = jnp.concatenate(columns, axis=1)
            field[p] = pltpu.roll(pltpu.roll(placed, width - shift_x, 0), length - shift_y, 1)

        early = reach * plane
        for phase, dst, amount in (
            (0, sums, count - 1), (1, held, early), (2, slope, early),
            (3, casorati, count - 1 - early), (4, shrunk, count - 1),
        ):
            if amount:
                all_of(dst, phase, it, amount).wait_send()
        return carry

    lax.fori_loop(0, iters, iteration, 0)
    out[...] = field[...]


def body(sizes, start_image, sensitivity, kspace, sampled, offsets):
    iters = offsets.shape[0]
    newton = 4
    _, _, width, length = start_image.shape
    coils = sensitivity.shape[0]
    count = sizes[0] * sizes[1] * sizes[2]
    ahead, back = dft_matrices(length)
    vmem = pl.BlockSpec(memory_space=pltpu.VMEM)
    hbm = pl.BlockSpec(memory_space=pltpu.HBM)
    messages = pltpu.VMEM((iters, count, 4, LANES), F32)
    run = pl.pallas_call(
        functools.partial(kernel, sizes, iters, newton),
        name="reconstruct",
        out_shape=pltpu.VMEM((2, width, length), F32),
        in_specs=[hbm] * 7,
        out_specs=vmem,
        scratch_shapes=[
            pltpu.SMEM(offsets.shape, jnp.int32),
            pltpu.VMEM(sensitivity.shape, BF16),
            pltpu.VMEM(kspace.shape[1:], BF16),
            pltpu.VMEM(sampled.shape[1:], jnp.int32),
            pltpu.VMEM(ahead.shape, BF16),
            pltpu.VMEM(back.shape, BF16),
            pltpu.VMEM((2, width, length), F32),
            pltpu.VMEM((2, width, length), F32),
            pltpu.VMEM((iters, 1, LANES), F32),
            pltpu.VMEM((iters, count, 1, LANES), F32),
            *[messages] * 8,
            pltpu.SemaphoreType.DMA((7,)),
            pltpu.SemaphoreType.DMA((5, iters)),
            pltpu.SemaphoreType.DMA((5, iters)),
        ],
        compiler_params=pltpu.CompilerParams(
            collective_id=0, has_side_effects=True, vmem_limit_bytes=67043328 - 409600
        ),
    )
    result = run(start_image[0], sensitivity, kspace[0], sampled[0], offsets, ahead, back)
    return result[None]


def solution(mesh):
    count = mesh.shape["tm"]
    sizes = (4, count // 8, 2) if count >= 64 else (2, count // 4, 2)
    both = ("cuts", "tm")
    placed = (
        P(both, None, None, None),
        P("cuts", None, None, None),
        P(both, None, None, None, None),
        P(both, None, None),
        P("cuts", None),
    )
    return jax.shard_map(
        functools.partial(body, sizes), mesh=mesh, in_specs=placed,
        out_specs=P(both, None, None, None), check_vma=False,
    )
```

```python
import functools
import math

import jax
import jax.numpy as jnp
import numpy as np
from jax import lax
from jax.experimental import pallas as pl
from jax.experimental.pallas import tpu as pltpu
from jax.sharding import PartitionSpec as P

BS = 16
LANES = 128
PER_TILE = LANES // BS
ROWS = 128
EARLY = 1
CLASSES = 2
shrink_ratio = 0.5
epsilon = 1e-06
F32 = jnp.float32
BF16 = jnp.bfloat16


def dft_matrices(length):
    indices = np.arange(length, dtype=np.int64)
    phases = (indices[:, None] * indices[None, :]) % length
    angles = phases.astype(np.float32) * np.float32(2.0 * math.pi / length)
    norm_scale = np.float32(1.0 / math.sqrt(length))
    cosine = jnp.asarray(np.cos(angles) * norm_scale).astype(BF16)
    sine = jnp.asarray(np.sin(angles) * norm_scale).astype(BF16)
    ahead = jnp.block([[cosine, -sine], [sine, cosine]])
    back = jnp.block([[cosine, sine], [-sine, cosine]])
    return ahead, back


def swap_groups(x):
    rows, lanes = x.shape
    x = x.reshape(rows // 8, 8, lanes)
    row = lax.broadcasted_iota(jnp.int32, x.shape, 1)
    lane = lax.broadcasted_iota(jnp.int32, x.shape, 2)
    for bit in (1, 2, 4):
        low_row = (row & bit) == 0
        low_lane = (lane & (bit * BS)) == 0
        other = pltpu.roll(x, bit, 1)
        if bit < 4:
            other = jnp.where(low_row, pltpu.roll(x, 8 - bit, 1), other)
        moved = pltpu.roll(other, bit * BS, 2)
        if bit < 4:
            moved = jnp.where(low_lane, pltpu.roll(other, lanes - bit * BS, 2), moved)
        x = jnp.where(low_row == low_lane, x, moved)
    return x.reshape(rows, lanes)


def kernel(
    sizes, iters, newton,
    start_hbm, sens_hbm, kspace_hbm, sampled_hbm, offsets_hbm, ahead_hbm, back_hbm,
    out,
    offsets, sens, kspace, sampled, ahead, back,
    field, grad, sums_src, sums, held_src, held, slope_src, slope,
    casorati_src, casorati, shrunk_src, shrunk,
    load_sems, send_sems, recv_sems,
):
    nx, nz, ny = sizes
    count = nx * nz * ny
    coils, _, width, length = sens.shape
    halves = length // LANES
    per_row = length // BS
    me = lax.axis_index("tm")
    my_x, my_z, my_y = me // (nz * ny), (me // ny) % nz, me % ny
    plane = nx * ny
    reach = min(EARLY, nz - 1)
    barrier = pltpu.get_barrier_semaphore()
    loads = [
        pltpu.make_async_copy(src, dst, load_sems.at[i])
        for i, (src, dst) in enumerate(
            (
                (sampled_hbm, sampled), (start_hbm, field), (sens_hbm, sens),
                (ahead_hbm, ahead), (kspace_hbm, kspace), (back_hbm, back),
                (offsets_hbm, offsets),
            )
        )
    ]
    for load in loads:
        load.start()

    def hop_of(i, flip=0):
        return nz // 2 + (1 - 2 * ((i + flip) % 2)) * ((i + 1) // 2)

    def peers(act, low=0, high=nz, classes=1):
        span = high - low
        across = sorted(range(nx), key=lambda d: -min(d, nx - d))

        def body(i, carry):
            for dx in across if classes == 1 else range(nx // classes):
                for dy in reversed(range(ny)):
                    flip = (dx * ny + dy) % 2 if low == 0 and high == nz else 0
                    z = (my_z + hop_of(low + i % span, flip)) % nz
                    if classes == 1:
                        x = (my_x + dx) % nx
                    else:
                        x = i // span + classes * dx
                    peer = (x * nz + z) * ny + (my_y + dy) % ny
                    if high < nz:
                        act(peer)
                    else:
                        pl.when(peer != me)(functools.partial(act, peer))
            return carry

        lax.fori_loop(0, classes * span, body, 0)

    peers(lambda peer: pl.semaphore_signal(barrier, inc=1, device_id={"tm": peer}))

    for load in loads[:4]:
        load.wait()
    weight = sampled[...].astype(F32)[:, None, :]

    def exchange(src_of, dst, phase, it, *which):
        def send(peer):
            pltpu.make_async_remote_copy(
                src_ref=src_of(peer),
                dst_ref=dst.at[it, me],
                send_sem=send_sems.at[phase, it],
                recv_sem=recv_sems.at[phase, it],
                device_id={"tm": peer},
            ).start()

        peers(send, *which)

    def all_of(dst, phase, it, amount):
        whole = dst.at[it, pl.ds(0, amount)]
        return pltpu.make_async_remote_copy(
            src_ref=whole, dst_ref=whole, send_sem=send_sems.at[phase, it],
            recv_sem=recv_sems.at[phase, it], device_id={"tm": me},
        )

    def iteration(it, carry):
        def chunk(c, acc):
            num, den = acc
            r0 = c * ROWS if isinstance(c, int) else pl.multiple_of(c * ROWS, ROWS)
            here = pl.ds(r0, ROWS)
            sr = sens[:, 0, here, :].astype(F32)
            si = sens[:, 1, here, :].astype(F32)

            def spectra(re, im):
                cr = (sr * re - si * im).astype(BF16).reshape(coils * ROWS, length)
                ci = (sr * im + si * re).astype(BF16).reshape(coils * ROWS, length)
                spec = jnp.dot(
                    jnp.concatenate([cr, ci], axis=1), ahead[...], preferred_element_type=F32
                )
                return (
                    spec[:, :length].reshape(coils, ROWS, length),
                    spec[:, length:].reshape(coils, ROWS, length),
                )

            fr, fi = spectra(field[0, here, :], field[1, here, :])

            @pl.when((it == 0) & (c == 0))
            def _():
                for load in loads[4:]:
                    load.wait()

            mr = (weight * (fr - kspace[:, 0, here, :].astype(F32))).astype(BF16)
            mi = (weight * (fi - kspace[:, 1, here, :].astype(F32))).astype(BF16)
            misfit = jnp.concatenate(
                [mr.reshape(coils * ROWS, length), mi.reshape(coils * ROWS, length)], axis=1
            )
            image = jnp.dot(misfit, back[...], preferred_element_type=F32)
            br = image[:, :length].reshape(coils, ROWS, length)
            bi = image[:, length:].reshape(coils, ROWS, length)
            gr = jnp.sum(sr * br + si * bi, axis=0)
            gi = jnp.sum(sr * bi - si * br, axis=0)
            grad[0, here, :] = gr
            grad[1, here, :] = gi
            num = num + jnp.sum((gr * gr + gi * gi).reshape(ROWS // 8, 8, length), axis=0)
            pr, pi = spectra(gr, gi)
            power = jnp.sum(weight * (pr * pr + pi * pi), axis=0)
            den = den + jnp.sum(power.reshape(ROWS // 8, 8, length), axis=0)
            return num, den

        zero = jnp.zeros((8, length), F32)
        if width == ROWS:
            num, den = chunk(0, (zero, zero))
        else:
            num, den = lax.fori_loop(0, width // ROWS, chunk, (zero, zero))

        def fold(v):
            v = jnp.sum(v, axis=0, keepdims=True)
            v = sum(v[:, h * LANES : (h + 1) * LANES] for h in range(halves))
            return v + pltpu.roll(v, LANES // 2, 1)

        first = lax.broadcasted_iota(jnp.int32, (1, LANES), 1) < LANES // 2
        mine = jnp.where(first, fold(num), fold(den))
        sums_src[it] = mine
        sums[it, me] = mine

        @pl.when(it == 0)
        def _():
            pl.semaphore_wait(barrier, count - 1)

        exchange(lambda peer: sums_src.at[it], sums, 0, it)

        shift_x, shift_y = offsets[it, 0], offsets[it, 1]

        def lay_out(image, dst):
            for p in range(2):
                rolled = pltpu.roll(pltpu.roll(image[p], shift_x, 0), shift_y, 1)
                for h in range(halves):
                    swapped = swap_groups(rolled[:, h * LANES : (h + 1) * LANES])
                    for g in range(width // 8):
                        u, q = g // 2, g % 2
                        rows = pl.ds(u * per_row + h * PER_TILE, PER_TILE)
                        dst[it, rows, p * 2 + q, :] = swapped[g * 8 : (g + 1) * 8, :]

        lay_out(field, held_src)
        if reach:
            exchange(lambda peer: held_src.at[it, peer], held, 1, it, 0, reach)
        lay_out(grad, slope_src)
        if reach:
            exchange(lambda peer: slope_src.at[it, peer], slope, 2, it, 0, reach)

        all_of(sums, 0, it, count - 1).wait_recv()
        total = jnp.sum(sums[it], axis=0)
        num_all = jnp.sum(jnp.where(first, total, 0.0), axis=1, keepdims=True)
        den_all = jnp.sum(jnp.where(first, 0.0, total), axis=1, keepdims=True)
        step_length = num_all / (den_all + epsilon)

        casorati_src[it] = held_src[it] - step_length[None] * slope_src[it]
        exchange(
            lambda peer: casorati_src.at[it, peer], casorati, 3, it, reach, nz, CLASSES
        )
        casorati[it, me] = casorati_src[it, me]
        if reach:
            all_of(held, 1, it, reach * plane).wait_recv()
            all_of(slope, 2, it, reach * plane).wait_recv()
        all_of(casorati, 3, it, count - 1 - reach * plane).wait_recv()
        for k in range(reach):
            z = (my_z + hop_of(k)) % nz
            for x in range(nx):
                rows = pl.ds((x * nz + z) * ny, ny)
                casorati[it, rows] = held[it, rows] - step_length[None] * slope[it, rows]

        parts = [casorati[it, :, j, :] for j in range(4)]
        full = jnp.concatenate(parts, axis=1)

        def split(a):
            high = a.astype(BF16)
            return high, (a - high.astype(F32)).astype(BF16)

        full_high, full_low = split(full)
        gram = lax.dot_general(
            jnp.concatenate([full_high, full_low, full_high], axis=1),
            jnp.concatenate([full_high, full_high, full_low], axis=1),
            (((1,), (1,)), ((), ())), preferred_element_type=F32,
        )
        frames = gram.shape[0]
        eye = (
            lax.broadcasted_iota(jnp.int32, gram.shape, 0)
            == lax.broadcasted_iota(jnp.int32, gram.shape, 1)
        ).astype(F32)
        trace = jnp.sum(jnp.sum(gram * eye, axis=1, keepdims=True), axis=0, keepdims=True)
        level = shrink_ratio * trace / frames + epsilon
        system = gram + level * eye
        bound = jnp.max(jnp.sum(jnp.abs(system), axis=1, keepdims=True), axis=0, keepdims=True)

        def times(a, b):
            a_high, a_low = split(a)
            b_high, b_low = split(b)
            return jnp.dot(
                jnp.concatenate([a_high, a_low, a_high], axis=1),
                jnp.concatenate([b_high, b_high, b_low], axis=0),
                preferred_element_type=F32,
            )

        residual = eye - system / bound
        product = eye + residual
        power = times(residual, residual)
        for step in range(newton - 2):
            both = times(jnp.concatenate([power, product], axis=0), power)
            product = product + both[frames:]
            power = both[:frames]
        product = product + times(product, power)
        scaled = product * (level / bound)
        result = full - times(scaled, full)
        for j in range(4):
            shrunk_src[it, :, j, :] = result[:, j * LANES : (j + 1) * LANES]

        exchange(lambda peer: shrunk_src.at[it, peer], shrunk, 4, it)
        shrunk[it, me] = shrunk_src[it, me]
        all_of(shrunk, 4, it, count - 1).wait_recv()

        for p in range(2):
            columns = []
            for h in range(halves):
                tiles = []
                for g in range(width // 8):
                    u, q = g // 2, g % 2
                    rows = pl.ds(u * per_row + h * PER_TILE, PER_TILE)
                    tiles.append(shrunk[it, rows, p * 2 + q, :])
                columns.append(swap_groups(jnp.concatenate(tiles, axis=0)))
            placed = jnp.concatenate(columns, axis=1)
            field[p] = pltpu.roll(pltpu.roll(placed, width - shift_x, 0), length - shift_y, 1)

        early = reach * plane
        for phase, dst, amount in (
            (0, sums, count - 1), (1, held, early), (2, slope, early),
            (3, casorati, count - 1 - early), (4, shrunk, count - 1),
        ):
            if amount:
                all_of(dst, phase, it, amount).wait_send()
        return carry

    lax.fori_loop(0, iters, iteration, 0)
    out[...] = field[...]


def body(sizes, start_image, sensitivity, kspace, sampled, offsets):
    iters = offsets.shape[0]
    newton = 4
    _, _, width, length = start_image.shape
    coils = sensitivity.shape[0]
    count = sizes[0] * sizes[1] * sizes[2]
    ahead, back = dft_matrices(length)
    vmem = pl.BlockSpec(memory_space=pltpu.VMEM)
    hbm = pl.BlockSpec(memory_space=pltpu.HBM)
    messages = pltpu.VMEM((iters, count, 4, LANES), F32)
    run = pl.pallas_call(
        functools.partial(kernel, sizes, iters, newton),
        name="reconstruct",
        out_shape=pltpu.VMEM((2, width, length), F32),
        in_specs=[hbm] * 7,
        out_specs=vmem,
        scratch_shapes=[
            pltpu.SMEM(offsets.shape, jnp.int32),
            pltpu.VMEM(sensitivity.shape, BF16),
            pltpu.VMEM(kspace.shape[1:], BF16),
            pltpu.VMEM(sampled.shape[1:], jnp.int32),
            pltpu.VMEM(ahead.shape, BF16),
            pltpu.VMEM(back.shape, BF16),
            pltpu.VMEM((2, width, length), F32),
            pltpu.VMEM((2, width, length), F32),
            pltpu.VMEM((iters, 1, LANES), F32),
            pltpu.VMEM((iters, count, 1, LANES), F32),
            *[messages] * 8,
            pltpu.SemaphoreType.DMA((7,)),
            pltpu.SemaphoreType.DMA((5, iters)),
            pltpu.SemaphoreType.DMA((5, iters)),
        ],
        compiler_params=pltpu.CompilerParams(
            collective_id=0, has_side_effects=True, vmem_limit_bytes=67043328 - 409600
        ),
    )
    result = run(start_image[0], sensitivity, kspace[0], sampled[0], offsets, ahead, back)
    return result[None]


def solution(mesh):
    count = mesh.shape["tm"]
    sizes = (4, count // 8, 2) if count >= 64 else (2, count // 4, 2)
    both = ("cuts", "tm")
    placed = (
        P(both, None, None, None),
        P("cuts", None, None, None),
        P(both, None, None, None, None),
        P(both, None, None),
        P("cuts", None),
    )
    return jax.shard_map(
        functools.partial(body, sizes), mesh=mesh, in_specs=placed,
        out_specs=P(both, None, None, None), check_vma=False,
    )
```
